32 devices in a mesh: dp: 4 (over x, core), tensor: 8 (over z, y).
Axes of the slice: x: 2, y: 2, z: 4, core: 2. Of those that a mesh axis runs over, the one named last changes fastest.
Arguments:
- activations: bfloat16 [2048, 28672], P('dp', 'tensor'), parts along dimension 0, may hold values from -6 to 6
- down_weight: bfloat16 [28672, 6144], P('tensor'), may hold values from -0.046875 to 0.046875
Outputs:
- projected: bfloat16 [2048, 6144], P(('dp', 'tensor')), parts along dimension 0
The draws below stay inside these ranges and needn't reach their ends.
There are 4 independent parts, one for each index of `dp`. The reference program is written for one: setup_inputs(seed, part) draws one part's arguments, and reference() takes and returns one part's arrays. A program takes and returns all parts, laid end to end along the dimension named above; an argument that names none is the same for every part. Nothing has to cross between parts.
All inputs are finite; a program needn't handle non-finite values.
Results may differ from the reference program's by a relative error of at most 0.015.
Values may be sent and summed in bfloat16 or wider, within the bound.
A program may use at most 128 MiB of HBM per device.

```python
import math
import jax
import jax.numpy as jnp
import numpy as np
from jax import lax

SYL = 1024
FF = 28672
DW = 6144
TOK = 512


def with_spikes(result, stream_key, source, target, blocks, factor):
    def block_of(position):
        return (jnp.arange(result.shape[position]) // (result.shape[position] // blocks)).reshape((-1,) + (1,) * (result.ndim - 1 - position))

    near = jax.random.permutation(stream_key, blocks)[block_of(target)]
    far = (block_of(target) + blocks // 2) % blocks
    return jnp.where((block_of(source) == near) | (block_of(source) == far), factor * result, result)


def level_of(stream_key, extent, cuts, smallest, top_value):
    loudness, own = 1.0, jax.random.fold_in(stream_key, 6)
    for position, parts in cuts:
        draws = jnp.exp(jax.random.uniform(jax.random.fold_in(own, position), (parts,), jnp.float32, smallest / len(cuts), top_value / len(cuts)))
        loudness = loudness * jnp.repeat(draws, extent[position] // parts).reshape([-1 if axis == position else 1 for axis in range(len(extent))])
    return loudness


def normal_values(own_key, dims, scale, limit, cuts=(), held_as=jnp.bfloat16):
    gain = level_of(own_key, dims, cuts, -0.22, 0.18) if cuts else 1.0
    values = jax.random.normal(own_key, dims, jnp.float32) * scale * gain
    return jnp.minimum(jnp.maximum(values, -limit), limit).astype(held_as)


def noise_with(own_key, extent, scale, reach, shards, heavy, dtype=jnp.bfloat16):
    result = scale * jax.random.normal(own_key, extent, jnp.float32)
    if shards:
        result = result * level_of(own_key, extent, shards, -0.22, 0.18)
    return jnp.clip(with_spikes(result, jax.random.fold_in(own_key, 3), *heavy), -reach, reach).astype(dtype)


def setup_inputs(seed: int = 0, part: int = 0) -> dict:
    arg_keys = jax.random.split(jax.random.key(seed), 3)
    own_keys = jax.random.split(jax.random.fold_in(arg_keys[2], part), 3)
    return {
        "activations": normal_values(own_keys[0], (TOK, FF), 1.0, 6.0, ((1, 8),)),
        "down_weight": noise_with(arg_keys[1], (FF, DW), FF ** -0.5, 0.046875, ((0, 8),), (0, 1, 8, 2.0)),
    }


def paley_matrix():
    modulus = 13
    residues = set((value * value % modulus for value in range(1, modulus)))
    jacobsthal = np.array([[0.0 if row_at == col_at else 1.0 if (col_at - row_at) % modulus in residues else -1.0 for col_at in range(modulus)] for row_at in range(modulus)])
    confer = np.zeros((14, 14))
    confer[0, 1:] = 1.0
    confer[1:, 0] = 1.0
    confer[1:, 1:] = jacobsthal
    return np.kron(confer, np.array([[1.0, 1.0], [1.0, -1.0]])) + np.kron(np.eye(14), np.array([[1.0, -1.0], [-1.0, -1.0]]))

def sylvester(order):
    matrix = np.ones((1, 1))
    while matrix.shape[0] < order:
        matrix = np.kron(matrix, np.array([[1.0, 1.0], [1.0, -1.0]]))
    return matrix

def quantize(rotated, largest):
    token_scale = jnp.maximum(largest, 1.0)
    levels = 7.0 * rotated / token_scale
    snapped = levels - jnp.sin(2.0 * math.pi * levels) / (2.0 * math.pi)
    return (snapped * token_scale / 7.0).astype(jnp.bfloat16)

def reference(activations, down_weight):
    count_rows = activations.shape[0]
    small_table = jnp.asarray(paley_matrix(), jnp.float32)
    power_table = jnp.asarray(sylvester(SYL), jnp.float32)
    values = activations.astype(jnp.float32).reshape(count_rows * SYL, 28)
    inner = jnp.dot(values, small_table, precision=lax.Precision.HIGHEST).reshape(count_rows, SYL, 28)
    outer = jnp.einsum('tji,jk->tki', inner, power_table, precision=lax.Precision.HIGHEST)
    rotated = outer.reshape(count_rows, FF) * (1.0 / math.sqrt(FF))
    largest = lax.optimization_barrier(jnp.max(jnp.abs(rotated), axis=1, keepdims=True))
    dequant = quantize(rotated, largest)
    return jnp.dot(dequant, down_weight, preferred_element_type=jnp.float32).astype(jnp.bfloat16)
```

```python
import functools
import math

import jax
import jax.numpy as jnp
import numpy as np
from jax import lax
from jax.experimental import pallas as pl
from jax.experimental.pallas import tpu as pltpu
from jax.sharding import PartitionSpec as P

INNER = 32
WEIGHT_SLOTS = 3


def paley_matrix():
    modulus = 13
    residues = set((value * value % modulus for value in range(1, modulus)))
    jacobsthal = np.array(
        [
            [
                (
                    0.0
                    if row_at == col_at
                    else 1.0 if (col_at - row_at) % modulus in residues else -1.0
                )
                for col_at in range(modulus)
            ]
            for row_at in range(modulus)
        ]
    )
    confer = np.zeros((14, 14))
    confer[0, 1:] = 1.0
    confer[1:, 0] = 1.0
    confer[1:, 1:] = jacobsthal
    return np.kron(confer, np.array([[1.0, 1.0], [1.0, -1.0]])) + np.kron(
        np.eye(14), np.array([[1.0, -1.0], [-1.0, -1.0]])
    )


def sylvester(order):
    matrix = np.ones((1, 1))
    while matrix.shape[0] < order:
        matrix = np.kron(matrix, np.array([[1.0, 1.0], [1.0, -1.0]]))
    return matrix


def sine_terms():
    series = np.polynomial.chebyshev.Chebyshev.interpolate(
        lambda square: np.sinc(2.0 * np.sqrt(np.maximum(square, 0.0))), 8, domain=[0.0, 0.25]
    )
    power = series.convert(kind=np.polynomial.Polynomial, domain=[-1, 1], window=[-1, 1])
    return [float(value) for value in power.coef]


def butterfly(values):
    step = 1
    while step < len(values):
        result = list(values)
        for at in range(len(values)):
            if not at & step:
                result[at] = values[at] + values[at + step]
                result[at + step] = values[at] - values[at + step]
        values, step = result, step * 2
    return values


def flipped(position, mask):
    result, bit = position, 1
    while bit <= mask:
        if mask & bit:
            result = result + (1 - 2 * ((position // bit) % 2)) * bit
        bit *= 2
    return result


def mirrored(position, groups):
    result, bit = 0, 1
    while bit < groups:
        result = result + ((position // bit) % 2) * (groups // 2 // bit)
        bit *= 2
    return result


def kernel(
    groups, chunks, tile, normal_scale, terms,
    act_ref, weight_ref, table_ref, out_ref,
    x_buf, rot, q_buf, d_buf, part, w_buf, *rest,
):
    stages = groups.bit_length() - 1
    recv_bufs = rest[:stages]
    (x_send, x_recv, own_sem, q_send, q_recv, r_send, r_recv, w_sem) = rest[stages:]
    me = lax.axis_index("tensor")
    rows = x_buf.shape[2]
    width = x_buf.shape[3]
    inner = table_ref.shape[0]
    subs = width // inner
    tiles = weight_ref.shape[1] // tile
    place = mirrored(me, groups)
    peers = [(mask, flipped(me, mask)) for mask in range(groups - 1, 0, -1)]

    def weight_copy(step):
        column = pl.multiple_of((step % tiles) * tile, 128)
        slot = step % WEIGHT_SLOTS
        return pltpu.make_async_copy(
            weight_ref.at[:, pl.ds(column, tile)], w_buf.at[slot], w_sem.at[slot]
        )

    def own_rows(chunk):
        first = pl.multiple_of(me * (chunks * rows) + chunk * rows, rows)
        return pltpu.make_async_copy(
            act_ref.at[pl.ds(first, rows), :], x_buf.at[chunk, me], own_sem.at[chunk]
        )

    def x_copy(chunk, mask, peer):
        first = pl.multiple_of(peer * (chunks * rows) + chunk * rows, rows)
        return pltpu.make_async_remote_copy(
            src_ref=act_ref.at[pl.ds(first, rows), :],
            dst_ref=x_buf.at[chunk, me],
            send_sem=x_send.at[chunk, mask],
            recv_sem=x_recv.at[chunk, mask],
            device_id={"tensor": peer},
            device_id_type=pl.DeviceIdType.MESH,
        )

    def q_copy(chunk, mask, peer):
        return pltpu.make_async_remote_copy(
            src_ref=q_buf.at[chunk, peer],
            dst_ref=d_buf.at[chunk, place],
            send_sem=q_send.at[chunk, mask],
            recv_sem=q_recv.at[chunk, mask],
            device_id={"tensor": peer},
            device_id_type=pl.DeviceIdType.MESH,
        )

    def half_at(stage):
        start, span, kept = 0, groups, 0
        for at in range(stage + 1):
            span //= 2
            start = kept
            bit = (me // (1 << at)) % 2
            kept = start + bit * span
            sent = start + (1 - bit) * span
        return kept, sent, span

    def r_copy(chunk, stage):
        kept, sent, span = half_at(stage)
        return pltpu.make_async_remote_copy(
            src_ref=part.at[chunk, pl.ds(sent, span)],
            dst_ref=recv_bufs[stage].at[chunk],
            send_sem=r_send.at[chunk, stage],
            recv_sem=r_recv.at[chunk, stage],
            device_id={"tensor": flipped(me, 1 << stage)},
            device_id_type=pl.DeviceIdType.MESH,
        )

    barrier = pltpu.get_barrier_semaphore()
    for mask, peer in peers:
        pl.semaphore_signal(
            barrier, inc=1, device_id={"tensor": peer}, device_id_type=pl.DeviceIdType.MESH
        )
    pl.semaphore_wait(barrier, groups - 1)

    for chunk in range(chunks):
        for mask, peer in peers:
            x_copy(chunk, mask, peer).start()
        own_rows(chunk).start()
    for step in range(WEIGHT_SLOTS):
        weight_copy(step).start()

    @pl.loop(0, chunks)
    def _(chunk):
        own_rows(chunk).wait()
        for mask, peer in peers:
            x_copy(chunk, mask, peer).wait_recv()
        for sub in range(subs):
            block = x_buf[chunk, :, :, sub * inner:(sub + 1) * inner]
            rot[sub] = jnp.dot(
                block.reshape(groups * rows, inner), table_ref[...],
                preferred_element_type=jnp.float32,
            ).reshape(groups, rows, inner)

        def mix(at, tops):
            column = pl.ds(pl.multiple_of(at * 128, 128), 128)
            result = []
            for index in range(rows // 8):
                line = pl.ds(index * 8, 8)
                values = butterfly(
                    [rot[sub, group, line, column] for group in range(groups) for sub in range(subs)]
                )
                top = tops[index]
                for block_at, value in enumerate(values):
                    rot[block_at % subs, block_at // subs, line, column] = value
                    top = jnp.maximum(top, jnp.abs(value))
                result.append(top)
            return tuple(result)

        tops = lax.fori_loop(
            0, inner // 128, mix,
            tuple(jnp.zeros((8, 128), jnp.float32) for _ in range(rows // 8)),
        )
        largest = jnp.concatenate([jnp.max(top, axis=1, keepdims=True) for top in tops], axis=0)
        token_scale = jnp.maximum(largest * normal_scale, 1.0)
        into = 7.0 * normal_scale / token_scale
        back = token_scale / 7.0

        @pl.loop(0, groups)
        def _(group):
            for sub in range(subs):
                levels = rot[sub, group] * into
                offset = levels - jnp.floor(levels + 0.5)
                square = offset * offset
                series = jnp.full_like(square, terms[-1])
                for term in terms[-2::-1]:
                    series = series * square + term
                q_buf[chunk, group, :, sub * inner:(sub + 1) * inner] = (
                    (levels - offset * series) * back
                ).astype(jnp.bfloat16)

        for mask, peer in peers:
            q_copy(chunk, mask, peer).start()
        d_buf[chunk, place] = q_buf[chunk, me]

    def reduce_stage(chunk, stage):
        r_copy(chunk, stage).wait_recv()
        kept, sent, span = half_at(stage)
        last = stage == stages - 1
        columns = part.shape[3] // 4

        @pl.loop(0, span * 4)
        def _(at):
            block, column = at // 4, pl.ds(pl.multiple_of((at % 4) * columns, 128), columns)
            total = (
                part[chunk, kept + block, :, column].astype(jnp.float32)
                + recv_bufs[stage][chunk, block, :, column].astype(jnp.float32)
            ).astype(jnp.bfloat16)
            if last:
                out_ref[pl.ds(chunk * rows, rows), column] = total
            else:
                part[chunk, kept + block, :, column] = total

        if not last:
            r_copy(chunk, stage + 1).start()

    for turn in range(chunks + stages):
        if turn < chunks:
            for mask, peer in peers:
                q_copy(turn, mask, peer).wait_recv()

            @pl.loop(0, tiles)
            def _(at):
                step = turn * tiles + at
                weight_copy(step).wait()
                part[turn, :, :, pl.ds(pl.multiple_of(at * tile, 128), tile)] = (
                    jnp.dot(
                        d_buf[turn].reshape(groups * rows, width),
                        w_buf[step % WEIGHT_SLOTS],
                        preferred_element_type=jnp.float32,
                    )
                    .astype(jnp.bfloat16)
                    .reshape(groups, rows, tile)
                )

                @pl.when(step + WEIGHT_SLOTS < chunks * tiles)
                def _():
                    weight_copy(step + WEIGHT_SLOTS).start()

            r_copy(turn, 0).start()
        for stage in range(stages):
            chunk = turn - 1 - stage
            if 0 <= chunk < chunks:
                reduce_stage(chunk, stage)

    for chunk in range(chunks):
        for mask, peer in peers:
            x_copy(chunk, mask, peer).wait_send()
            q_copy(chunk, mask, peer).wait_send()
        for stage in range(stages):
            r_copy(chunk, stage).wait_send()


def shards(activations, down_weight):
    count_rows, width = activations.shape
    features = down_weight.shape[1]
    groups = lax.axis_size("tensor")
    stages = groups.bit_length() - 1
    own = count_rows // groups
    rows = 16
    chunks = own // rows
    tile = 512
    table = jnp.asarray(np.kron(sylvester(INNER), paley_matrix()), jnp.bfloat16)
    inner = table.shape[0]
    bf16, dma = jnp.bfloat16, pltpu.SemaphoreType.DMA
    body = functools.partial(
        kernel, groups, chunks, tile, 1.0 / math.sqrt(width * groups), sine_terms()
    )
    return pl.pallas_call(
        body,
        out_shape=jax.ShapeDtypeStruct((own, features), bf16),
        in_specs=[
            pl.BlockSpec(memory_space=pl.ANY),
            pl.BlockSpec(memory_space=pl.ANY),
            pl.BlockSpec(memory_space=pltpu.VMEM),
        ],
        out_specs=pl.BlockSpec(memory_space=pltpu.VMEM),
        scratch_shapes=[
            pltpu.VMEM((chunks, groups, rows, width), bf16),
            pltpu.VMEM((width // inner, groups, rows, inner), jnp.float32),
            pltpu.VMEM((chunks, groups, rows, width), bf16),
            pltpu.VMEM((chunks, groups, rows, width), bf16),
            pltpu.VMEM((chunks, groups, rows, features), bf16),
            pltpu.VMEM((WEIGHT_SLOTS, width, tile), bf16),
        ]
        + [
            pltpu.VMEM((chunks, groups >> (stage + 1), rows, features), bf16)
            for stage in range(stages)
        ]
        + [
            dma((chunks, groups)),
            dma((chunks, groups)),
            dma((chunks,)),
            dma((chunks, groups)),
            dma((chunks, groups)),
            dma((chunks, stages)),
            dma((chunks, stages)),
            dma((WEIGHT_SLOTS,)),
        ],
        compiler_params=pltpu.CompilerParams(
            collective_id=0, has_side_effects=True, vmem_limit_bytes=60 * 1024 * 1024
        ),
        name="rotate_quantize_project",
    )(activations, down_weight, table)


def solution(mesh):
    placed = (P("dp", "tensor"), P("tensor", None))
    return jax.shard_map(
        shards, mesh=mesh, in_specs=placed, out_specs=P(("dp", "tensor"), None), check_vma=False
    )
```

```python
import functools
import math

import jax
import jax.numpy as jnp
import numpy as np
from jax import lax
from jax.experimental import pallas as pl
from jax.experimental.pallas import tpu as pltpu
from jax.sharding import PartitionSpec as P

INNER = 32
WEIGHT_SLOTS = 8
SECTIONS = 6
AHEAD = 2


def paley_matrix():
    modulus = 13
    residues = set((value * value % modulus for value in range(1, modulus)))
    jacobsthal = np.array(
        [
            [
                (
                    0.0
                    if row_at == col_at
                    else 1.0 if (col_at - row_at) % modulus in residues else -1.0
                )
                for col_at in range(modulus)
            ]
            for row_at in range(modulus)
        ]
    )
    confer = np.zeros((14, 14))
    confer[0, 1:] = 1.0
    confer[1:, 0] = 1.0
    confer[1:, 1:] = jacobsthal
    return np.kron(confer, np.array([[1.0, 1.0], [1.0, -1.0]])) + np.kron(
        np.eye(14), np.array([[1.0, -1.0], [-1.0, -1.0]])
    )


def sylvester(order):
    matrix = np.ones((1, 1))
    while matrix.shape[0] < order:
        matrix = np.kron(matrix, np.array([[1.0, 1.0], [1.0, -1.0]]))
    return matrix


def sine_terms():
    series = np.polynomial.chebyshev.Chebyshev.interpolate(
        lambda square: np.sinc(2.0 * np.sqrt(np.maximum(square, 0.0))), 8, domain=[0.0, 0.25]
    )
    power = series.convert(kind=np.polynomial.Polynomial, domain=[-1, 1], window=[-1, 1])
    return [float(value) for value in power.coef]


def butterfly(values):
    step = 1
    while step < len(values):
        result = list(values)
        for at in range(len(values)):
            if not at & step:
                result[at] = values[at] + values[at + step]
                result[at + step] = values[at] - values[at + step]
        values, step = result, step * 2
    return values


def flipped(position, mask):
    result, bit = position, 1
    while bit <= mask:
        if mask & bit:
            result = result + (1 - 2 * ((position // bit) % 2)) * bit
        bit *= 2
    return result


def mirrored(position, groups):
    result, bit = 0, 1
    while bit < groups:
        result = result + ((position // bit) % 2) * (groups // 2 // bit)
        bit *= 2
    return result


def kernel(
    groups, chunks, tile, normal_scale, terms,
    act_ref, weight_ref, table_ref, out_ref,
    x_buf, rot, q_buf, d_buf, part, w_buf, *rest,
):
    stages = groups.bit_length() - 1
    recv_bufs = rest[:stages]
    (x_send, x_recv, own_sem, q_send, q_recv, r_send, r_recv, w_sem) = rest[stages:]
    me = lax.axis_index("tensor")
    rows = x_buf.shape[2]
    width = x_buf.shape[3]
    inner = table_ref.shape[0]
    subs = width // inner
    tiles = weight_ref.shape[1] // tile
    section_tiles = tiles // SECTIONS
    section_width = section_tiles * tile
    place = mirrored(me, groups)
    peers = [(mask, flipped(me, mask)) for mask in range(groups - 1, 0, -1)]

    def weight_copy(step):
        column = pl.multiple_of((step % tiles) * tile, 128)
        slot = step % WEIGHT_SLOTS
        return pltpu.make_async_copy(
            weight_ref.at[:, pl.ds(column, tile)], w_buf.at[slot], w_sem.at[slot]
        )

    def own_rows(chunk):
        first = pl.multiple_of(me * (chunks * rows) + chunk * rows, rows)
        return pltpu.make_async_copy(
            act_ref.at[pl.ds(first, rows), :], x_buf.at[chunk, me], own_sem.at[chunk]
        )

    def x_copy(chunk, mask, peer):
        first = pl.multiple_of(peer * (chunks * rows) + chunk * rows, rows)
        return pltpu.make_async_remote_copy(
            src_ref=act_ref.at[pl.ds(first, rows), :],
            dst_ref=x_buf.at[chunk, me],
            send_sem=x_send.at[chunk, mask],
            recv_sem=x_recv.at[chunk, mask],
            device_id={"tensor": peer},
            device_id_type=pl.DeviceIdType.MESH,
        )

    def q_copy(chunk, mask, peer):
        return pltpu.make_async_remote_copy(
            src_ref=q_buf.at[chunk, peer],
            dst_ref=d_buf.at[chunk, place],
            send_sem=q_send.at[chunk, mask],
            recv_sem=q_recv.at[chunk, mask],
            device_id={"tensor": peer},
            device_id_type=pl.DeviceIdType.MESH,
        )

    def half_at(stage):
        start, span, kept = 0, groups, 0
        for at in range(stage + 1):
            span //= 2
            start = kept
            bit = (me // (1 << at)) % 2
            kept = start + bit * span
            sent = start + (1 - bit) * span
        return kept, sent, span

    def r_copy(chunk, stage, section):
        kept, sent, span = half_at(stage)
        column = pl.ds(section * section_width, section_width)
        return pltpu.make_async_remote_copy(
            src_ref=part.at[chunk, pl.ds(sent, span), :, column],
            dst_ref=recv_bufs[stage].at[chunk, :, :, column],
            send_sem=r_send.at[chunk, stage, section],
            recv_sem=r_recv.at[chunk, stage, section],
            device_id={"tensor": flipped(me, 1 << stage)},
            device_id_type=pl.DeviceIdType.MESH,
        )

    barrier = pltpu.get_barrier_semaphore()
    for mask, peer in peers:
        pl.semaphore_signal(
            barrier, inc=1, device_id={"tensor": peer}, device_id_type=pl.DeviceIdType.MESH
        )
    pl.semaphore_wait(barrier, groups - 1)

    def exchange(chunk):
        for mask, peer in peers:
            x_copy(chunk, mask, peer).start()
        own_rows(chunk).start()

    for chunk in range(min(AHEAD, chunks)):
        exchange(chunk)
    for step in range(WEIGHT_SLOTS):
        weight_copy(step).start()

    def rotate(chunk):
        for sub in range(subs):
            block = x_buf[chunk, :, :, sub * inner:(sub + 1) * inner]
            rot[sub] = jnp.dot(
                block.reshape(groups * rows, inner), table_ref[...],
                preferred_element_type=jnp.float32,
            ).reshape(groups, rows, inner)

        def mix(at, tops):
            column = pl.ds(pl.multiple_of(at * 128, 128), 128)
            result = []
            for index in range(rows // 8):
                line = pl.ds(index * 8, 8)
                values = butterfly(
                    [rot[sub, group, line, column] for group in range(groups) for sub in range(subs)]
                )
                top = tops[index]
                for block_at, value in enumerate(values):
                    rot[block_at % subs, block_at // subs, line, column] = value
                    top = jnp.maximum(top, jnp.abs(value))
                result.append(top)
            return tuple(result)

        tops = lax.fori_loop(
            0, inner // 128, mix,
            tuple(jnp.zeros((8, 128), jnp.float32) for _ in range(rows // 8)),
        )
        largest = jnp.concatenate([jnp.max(top, axis=1, keepdims=True) for top in tops], axis=0)
        token_scale = jnp.maximum(largest * normal_scale, 1.0)
        into = 7.0 * normal_scale / token_scale
        back = token_scale / 7.0

        @pl.loop(0, groups)
        def _(group):
            for sub in range(subs):
                levels = rot[sub, group] * into
                offset = levels - jnp.floor(levels + 0.5)
                square = offset * offset
                series = jnp.full_like(square, terms[-1])
                for term in terms[-2::-1]:
                    series = series * square + term
                q_buf[chunk, group, :, sub * inner:(sub + 1) * inner] = (
                    (levels - offset * series) * back
                ).astype(jnp.bfloat16)

    def finish_tokens(chunk):
        own_rows(chunk).wait()
        for mask, peer in peers:
            x_copy(chunk, mask, peer).wait_recv()
        rotate(chunk)
        for mask, peer in peers:
            q_copy(chunk, mask, peer).start()
        d_buf[chunk, place] = q_buf[chunk, me]
        if chunk + AHEAD < chunks:
            exchange(chunk + AHEAD)

    def reduce_stage(chunk, stage, section):
        r_copy(chunk, stage, section).wait_recv()
        kept, sent, span = half_at(stage)
        last = stage == stages - 1
        piece = section_width // 2

        @pl.loop(0, span * 2)
        def _(at):
            block = at // 2
            column = pl.ds(pl.multiple_of(section * section_width + (at % 2) * piece, 128), piece)
            total = (
                part[chunk, kept + block, :, column].astype(jnp.float32)
                + recv_bufs[stage][chunk, block, :, column].astype(jnp.float32)
            ).astype(jnp.bfloat16)
            if last:
                out_ref[pl.ds(chunk * rows, rows), column] = total
            else:
                part[chunk, kept + block, :, column] = total

        if not last:
            r_copy(chunk, stage + 1, section).start()

    def project(chunk):
        for mask, peer in peers:
            q_copy(chunk, mask, peer).wait_recv()
        for section in range(SECTIONS):
            @pl.loop(section * section_tiles, (section + 1) * section_tiles)
            def _(at):
                step = chunk * tiles + at
                weight_copy(step).wait()
                part[chunk, :, :, pl.ds(pl.multiple_of(at * tile, 128), tile)] = (
                    jnp.dot(
                        d_buf[chunk].reshape(groups * rows, width),
                        w_buf[step % WEIGHT_SLOTS],
                        preferred_element_type=jnp.float32,
                    )
                    .astype(jnp.bfloat16)
                    .reshape(groups, rows, tile)
                )

                @pl.when(step + WEIGHT_SLOTS < chunks * tiles)
                def _():
                    weight_copy(step + WEIGHT_SLOTS).start()

            r_copy(chunk, 0, section).start()

    for chunk in range(min(AHEAD, chunks)):
        finish_tokens(chunk)
    for turn in range(chunks + stages):
        if turn < chunks:
            project(turn)
        for stage in range(stages):
            chunk = turn - 1 - stage
            if 0 <= chunk < chunks:
                for section in range(SECTIONS):
                    reduce_stage(chunk, stage, section)
        if AHEAD <= turn + AHEAD < chunks:
            finish_tokens(turn + AHEAD)

    for chunk in range(chunks):
        for mask, peer in peers:
            x_copy(chunk, mask, peer).wait_send()
            q_copy(chunk, mask, peer).wait_send()
        for stage in range(stages):
            for section in range(SECTIONS):
                r_copy(chunk, stage, section).wait_send()


def shards(activations, down_weight):
    count_rows, width = activations.shape
    features = down_weight.shape[1]
    groups = lax.axis_size("tensor")
    stages = groups.bit_length() - 1
    own = count_rows // groups
    rows = 16
    chunks = own // rows
    tile = 512
    table = jnp.asarray(np.kron(sylvester(INNER), paley_matrix()), jnp.bfloat16)
    inner = table.shape[0]
    bf16, dma = jnp.bfloat16, pltpu.SemaphoreType.DMA
    body = functools.partial(
        kernel, groups, chunks, tile, 1.0 / math.sqrt(width * groups), sine_terms()
    )
    return pl.pallas_call(
        body,
        out_shape=jax.ShapeDtypeStruct((own, features), bf16),
        in_specs=[
            pl.BlockSpec(memory_space=pl.ANY),
            pl.BlockSpec(memory_space=pl.ANY),
            pl.BlockSpec(memory_space=pltpu.VMEM),
        ],
        out_specs=pl.BlockSpec(memory_space=pltpu.VMEM),
        scratch_shapes=[
            pltpu.VMEM((chunks, groups, rows, width), bf16),
            pltpu.VMEM((width // inner, groups, rows, inner), jnp.float32),
            pltpu.VMEM((chunks, groups, rows, width), bf16),
            pltpu.VMEM((chunks, groups, rows, width), bf16),
            pltpu.VMEM((chunks, groups, rows, features), bf16),
            pltpu.VMEM((WEIGHT_SLOTS, width, tile), bf16),
        ]
        + [
            pltpu.VMEM((chunks, groups >> (stage + 1), rows, features), bf16)
            for stage in range(stages)
        ]
        + [
            dma((chunks, groups)),
            dma((chunks, groups)),
            dma((chunks,)),
            dma((chunks, groups)),
            dma((chunks, groups)),
            dma((chunks, stages, SECTIONS)),
            dma((chunks, stages, SECTIONS)),
            dma((WEIGHT_SLOTS,)),
        ],
        compiler_params=pltpu.CompilerParams(
            collective_id=0, has_side_effects=True, vmem_limit_bytes=60 * 1024 * 1024
        ),
        name="rotate_quantize_project",
    )(activations, down_weight, table)


def solution(mesh):
    placed = (P("dp", "tensor"), P("tensor", None))
    return jax.shard_map(
        shards, mesh=mesh, in_specs=placed, out_specs=P(("dp", "tensor"), None), check_vma=False
    )
```

```python
import functools
import math

import jax
import jax.numpy as jnp
import numpy as np
from jax import lax
from jax.experimental import pallas as pl
from jax.experimental.pallas import tpu as pltpu
from jax.sharding import PartitionSpec as P

INNER = 32
WEIGHT_SLOTS = 8
SECTIONS = 6
AHEAD = 2


def paley_matrix():
    modulus = 13
    residues = set((value * value % modulus for value in range(1, modulus)))
    jacobsthal = np.array(
        [
            [
                (
                    0.0
                    if row_at == col_at
                    else 1.0 if (col_at - row_at) % modulus in residues else -1.0
                )
                for col_at in range(modulus)
            ]
            for row_at in range(modulus)
        ]
    )
    confer = np.zeros((14, 14))
    confer[0, 1:] = 1.0
    confer[1:, 0] = 1.0
    confer[1:, 1:] = jacobsthal
    return np.kron(confer, np.array([[1.0, 1.0], [1.0, -1.0]])) + np.kron(
        np.eye(14), np.array([[1.0, -1.0], [-1.0, -1.0]])
    )


def sylvester(order):
    matrix = np.ones((1, 1))
    while matrix.shape[0] < order:
        matrix = np.kron(matrix, np.array([[1.0, 1.0], [1.0, -1.0]]))
    return matrix


def sine_terms():
    series = np.polynomial.chebyshev.Chebyshev.interpolate(
        lambda square: np.sinc(2.0 * np.sqrt(np.maximum(square, 0.0))), 8, domain=[0.0, 0.25]
    )
    power = series.convert(kind=np.polynomial.Polynomial, domain=[-1, 1], window=[-1, 1])
    return [float(value) for value in power.coef]


def butterfly(values):
    step = 1
    while step < len(values):
        result = list(values)
        for at in range(len(values)):
            if not at & step:
                result[at] = values[at] + values[at + step]
                result[at + step] = values[at] - values[at + step]
        values, step = result, step * 2
    return values


def flipped(position, mask):
    result, bit = position, 1
    while bit <= mask:
        if mask & bit:
            result = result + (1 - 2 * ((position // bit) % 2)) * bit
        bit *= 2
    return result


def mirrored(position, groups):
    result, bit = 0, 1
    while bit < groups:
        result = result + ((position // bit) % 2) * (groups // 2 // bit)
        bit *= 2
    return result


def kernel(
    groups, chunks, tile, normal_scale, terms,
    act_ref, weight_ref, table_ref, out_ref,
    x_buf, rot, q_buf, d_buf, part, w_buf, *rest,
):
    stages = groups.bit_length() - 1
    recv_bufs = rest[:stages]
    (x_send, x_recv, own_sem, q_send, q_recv, r_send, r_recv, w_sem) = rest[stages:]
    me = lax.axis_index("tensor")
    rows = x_buf.shape[2]
    width = x_buf.shape[3]
    inner = table_ref.shape[0]
    subs = width // inner
    tiles = weight_ref.shape[1] // tile
    section_tiles = tiles // SECTIONS
    section_width = section_tiles * tile
    place = mirrored(me, groups)
    peers = [(mask, flipped(me, mask)) for mask in range(groups - 1, 0, -1)]

    def weight_copy(step):
        column = pl.multiple_of((step % tiles) * tile, 128)
        slot = step % WEIGHT_SLOTS
        return pltpu.make_async_copy(
            weight_ref.at[:, pl.ds(column, tile)], w_buf.at[slot], w_sem.at[slot]
        )

    def own_rows(chunk):
        first = pl.multiple_of(me * (chunks * rows) + chunk * rows, rows)
        return pltpu.make_async_copy(
            act_ref.at[pl.ds(first, rows), :], x_buf.at[chunk, me], own_sem.at[chunk]
        )

    def x_copy(chunk, mask, peer):
        first = pl.multiple_of(peer * (chunks * rows) + chunk * rows, rows)
        return pltpu.make_async_remote_copy(
            src_ref=act_ref.at[pl.ds(first, rows), :],
            dst_ref=x_buf.at[chunk, me],
            send_sem=x_send.at[chunk, mask],
            recv_sem=x_recv.at[chunk, mask],
            device_id={"tensor": peer},
            device_id_type=pl.DeviceIdType.MESH,
        )

    def q_copy(chunk, mask, peer):
        return pltpu.make_async_remote_copy(
            src_ref=q_buf.at[chunk, peer],
            dst_ref=d_buf.at[chunk, place],
            send_sem=q_send.at[chunk, mask],
            recv_sem=q_recv.at[chunk, mask],
            device_id={"tensor": peer},
            device_id_type=pl.DeviceIdType.MESH,
        )

    def half_at(stage):
        start, span, kept = 0, groups, 0
        for at in range(stage + 1):
            span //= 2
            start = kept
            bit = (me // (1 << at)) % 2
            kept = start + bit * span
            sent = start + (1 - bit) * span
        return kept, sent, span

    def r_copy(chunk, stage, section):
        kept, sent, span = half_at(stage)
        column = pl.ds(section * section_width, section_width)
        return pltpu.make_async_remote_copy(
            src_ref=part.at[chunk, pl.ds(sent, span), :, column],
            dst_ref=recv_bufs[stage].at[chunk, :, :, column],
            send_sem=r_send.at[chunk, stage, section],
            recv_sem=r_recv.at[chunk, stage, section],
            device_id={"tensor": flipped(me, 1 << stage)},
            device_id_type=pl.DeviceIdType.MESH,
        )

    barrier = pltpu.get_barrier_semaphore()
    for mask, peer in peers:
        pl.semaphore_signal(
            barrier, inc=1, device_id={"tensor": peer}, device_id_type=pl.DeviceIdType.MESH
        )
    pl.semaphore_wait(barrier, groups - 1)

    def exchange(chunk):
        for mask, peer in peers:
            x_copy(chunk, mask, peer).start()
        own_rows(chunk).start()

    for chunk in range(min(AHEAD, chunks)):
        exchange(chunk)
    for step in range(WEIGHT_SLOTS):
        weight_copy(step).start()

    def rotate(chunk):
        for sub in range(subs):
            block = x_buf[chunk, :, :, sub * inner:(sub + 1) * inner]
            rot[sub] = jnp.dot(
                block.reshape(groups * rows, inner), table_ref[...],
                preferred_element_type=jnp.float32,
            ).reshape(groups, rows, inner)

        def mix(at, tops):
            column = pl.ds(pl.multiple_of(at * 128, 128), 128)
            result = []
            for index in range(rows // 8):
                line = pl.ds(index * 8, 8)
                values = butterfly(
                    [rot[sub, group, line, column] for group in range(groups) for sub in range(subs)]
                )
                top = tops[index]
                for block_at, value in enumerate(values):
                    rot[block_at % subs, block_at // subs, line, column] = value
                    top = jnp.maximum(top, jnp.abs(value))
                result.append(top)
            return tuple(result)

        tops = lax.fori_loop(
            0, inner // 128, mix,
            tuple(jnp.zeros((8, 128), jnp.float32) for _ in range(rows // 8)),
        )
        largest = jnp.concatenate([jnp.max(top, axis=1, keepdims=True) for top in tops], axis=0)
        token_scale = jnp.maximum(largest * normal_scale, 1.0)
        into = 7.0 * normal_scale / token_scale
        back = token_scale / 7.0

        @pl.loop(0, groups)
        def _(group):
            for sub in range(subs):
                levels = rot[sub, group] * into
                offset = levels - jnp.floor(levels + 0.5)
                square = offset * offset
                series = jnp.full_like(square, terms[-1])
                for term in terms[-2::-1]:
                    series = series * square + term
                q_buf[chunk, group, :, sub * inner:(sub + 1) * inner] = (
                    (levels - offset * series) * back
                ).astype(jnp.bfloat16)

    def finish_tokens(chunk):
        own_rows(chunk).wait()
        for mask, peer in peers:
            x_copy(chunk, mask, peer).wait_recv()
        rotate(chunk)
        for mask, peer in peers:
            q_copy(chunk, mask, peer).start()
        d_buf[chunk, place] = q_buf[chunk, me]
        if chunk + AHEAD < chunks:
            exchange(chunk + AHEAD)

    def reduce_stage(chunk, stage, section):
        r_copy(chunk, stage, section).wait_recv()
        kept, sent, span = half_at(stage)
        last = stage == stages - 1
        piece = section_width // 2

        @pl.loop(0, span * 2)
        def _(at):
            block = at // 2
            column = pl.ds(pl.multiple_of(section * section_width + (at % 2) * piece, 128), piece)
            total = (
                part[chunk, kept + block, :, column].astype(jnp.float32)
                + recv_bufs[stage][chunk, block, :, column].astype(jnp.float32)
            ).astype(jnp.bfloat16)
            if last:
                out_ref[pl.ds(chunk * rows, rows), column] = total
            else:
                part[chunk, kept + block, :, column] = total

        if not last:
            r_copy(chunk, stage + 1, section).start()

    def project(chunk):
        for mask, peer in peers:
            q_copy(chunk, mask, peer).wait_recv()
        for section in range(SECTIONS):
            @pl.loop(section * section_tiles, (section + 1) * section_tiles)
            def _(at):
                step = chunk * tiles + at
                weight_copy(step).wait()
                part[chunk, :, :, pl.ds(pl.multiple_of(at * tile, 128), tile)] = (
                    jnp.dot(
                        d_buf[chunk].reshape(groups * rows, width),
                        w_buf[step % WEIGHT_SLOTS],
                        preferred_element_type=jnp.float32,
                    )
                    .astype(jnp.bfloat16)
                    .reshape(groups, rows, tile)
                )

                @pl.when(step + WEIGHT_SLOTS < chunks * tiles)
                def _():
                    weight_copy(step + WEIGHT_SLOTS).start()

            r_copy(chunk, 0, section).start()

    for chunk in range(min(AHEAD, chunks)):
        finish_tokens(chunk)
    for turn in range(chunks + stages):
        if turn < chunks:
            project(turn)
        for section in range(SECTIONS):
            for stage in range(stages - 1, -1, -1):
                chunk = turn - 1 - stage
                if 0 <= chunk < chunks:
                    reduce_stage(chunk, stage, section)
        if AHEAD <= turn + AHEAD < chunks:
            finish_tokens(turn + AHEAD)

    for chunk in range(chunks):
        for mask, peer in peers:
            x_copy(chunk, mask, peer).wait_send()
            q_copy(chunk, mask, peer).wait_send()
        for stage in range(stages):
            for section in range(SECTIONS):
                r_copy(chunk, stage, section).wait_send()


def shards(activations, down_weight):
    count_rows, width = activations.shape
    features = down_weight.shape[1]
    groups = lax.axis_size("tensor")
    stages = groups.bit_length() - 1
    own = count_rows // groups
    rows = 16
    chunks = own // rows
    tile = 512
    table = jnp.asarray(np.kron(sylvester(INNER), paley_matrix()), jnp.bfloat16)
    inner = table.shape[0]
    bf16, dma = jnp.bfloat16, pltpu.SemaphoreType.DMA
    body = functools.partial(
        kernel, groups, chunks, tile, 1.0 / math.sqrt(width * groups), sine_terms()
    )
    return pl.pallas_call(
        body,
        out_shape=jax.ShapeDtypeStruct((own, features), bf16),
        in_specs=[
            pl.BlockSpec(memory_space=pl.ANY),
            pl.BlockSpec(memory_space=pl.ANY),
            pl.BlockSpec(memory_space=pltpu.VMEM),
        ],
        out_specs=pl.BlockSpec(memory_space=pltpu.VMEM),
        scratch_shapes=[
            pltpu.VMEM((chunks, groups, rows, width), bf16),
            pltpu.VMEM((width // inner, groups, rows, inner), jnp.float32),
            pltpu.VMEM((chunks, groups, rows, width), bf16),
            pltpu.VMEM((chunks, groups, rows, width), bf16),
            pltpu.VMEM((chunks, groups, rows, features), bf16),
            pltpu.VMEM((WEIGHT_SLOTS, width, tile), bf16),
        ]
        + [
            pltpu.VMEM((chunks, groups >> (stage + 1), rows, features), bf16)
            for stage in range(stages)
        ]
        + [
            dma((chunks, groups)),
            dma((chunks, groups)),
            dma((chunks,)),
            dma((chunks, groups)),
            dma((chunks, groups)),
            dma((chunks, stages, SECTIONS)),
            dma((chunks, stages, SECTIONS)),
            dma((WEIGHT_SLOTS,)),
        ],
        compiler_params=pltpu.CompilerParams(
            collective_id=0, has_side_effects=True, vmem_limit_bytes=60 * 1024 * 1024
        ),
        name="rotate_quantize_project",
    )(activations, down_weight, table)


def solution(mesh):
    placed = (P("dp", "tensor"), P("tensor", None))
    return jax.shard_map(
        shards, mesh=mesh, in_specs=placed, out_specs=P(("dp", "tensor"), None), check_vma=False
    )
```
